16 devices in a mesh: rep: 1, dp: 16 (over x, y, z, core).
Axes of the slice: x: 2, y: 2, z: 2, core: 2. Of those that a mesh axis runs over, the one named last changes fastest.
Arguments:
- x: bfloat16 [16, 2048, 768], P(('rep', 'dp'))
- dy: bfloat16 [16, 2048, 768], P(('rep', 'dp'))
- w_gate: bfloat16 [2, 768, 6144], replicated
- w_up: bfloat16 [2, 768, 6144], replicated
- w_down: bfloat16 [2, 6144, 768], replicated
- m_w_gate: float32 [2, 768, 6144], replicated
- m_w_up: float32 [2, 768, 6144], replicated
- m_w_down: float32 [2, 6144, 768], replicated
- v_w_gate: float32 [2, 768, 6144], replicated
- v_w_up: float32 [2, 768, 6144], replicated
- v_w_down: float32 [2, 6144, 768], replicated
Outputs:
- output 1: bfloat16 [2, 768, 6144], P('rep')
- output 2: bfloat16 [2, 768, 6144], P('rep')
- output 3: bfloat16 [2, 6144, 768], P('rep')
- output 4: float32 [2, 768, 6144], P('rep')
- output 5: float32 [2, 768, 6144], P('rep')
- output 6: float32 [2, 6144, 768], P('rep')
- output 7: float32 [2, 768, 6144], P('rep')
- output 8: float32 [2, 768, 6144], P('rep')
- output 9: float32 [2, 6144, 768], P('rep')
All inputs are finite; a program needn't handle non-finite values.
Results may differ from the reference program's by a relative error of at most 0.022.
Values are sent between devices in bfloat16 or wider.
A program may use at most 3 GiB of HBM per device.

```python
import jax
import jax.numpy as jnp
from jax import lax

SEQUENCES = 16
TOKENS = 2048
D = 768
FF = 6144
LAYERS = 2
NAMES = ("w_gate", "w_up", "w_down")
SHAPES = {"w_gate": (LAYERS, D, FF), "w_up": (LAYERS, D, FF), "w_down": (LAYERS, FF, D)}


def bump(key, n, height):
    away = (jnp.arange(n, dtype=jnp.int32) - jax.random.randint(key, (), 0, n, jnp.int32)) % n
    return jnp.where(away < n // 8, height, 1.0)


def together(key, own, strength):
    shared = jax.random.normal(key, own.shape[1:], jnp.float32)
    return (own + strength * shared) * lax.rsqrt(1 + strength * strength)


def setup_inputs(seed: int = 0, part: int = 0) -> dict:
    kx, kdy, ka, kb, kz, kf, kh, kl, *keys = jax.random.split(jax.random.key(seed), 8 + 3 * len(NAMES))
    kx, kdy, ka, kb = (jax.random.fold_in(k, part) for k in (kx, kdy, ka, kb))
    kw, km, kv = (keys[i::3] for i in range(3))
    shape = (SEQUENCES, TOKENS, D)
    much_x, much_dy = jax.random.uniform(kz, (2,), jnp.float32, 0.0, 1.0)
    loud = 2.0 ** jax.random.uniform(jax.random.fold_in(kz, 1), (), jnp.float32, -1.0, 2.0)
    layers = 2.0 ** jax.random.uniform(kl, (LAYERS, 1, 1), jnp.float32, -1.0, 1.0)
    x = together(ka, jax.random.normal(kx, shape, jnp.float32), much_x) * bump(kf, D, 4.0)
    dy = together(kb, jax.random.normal(kdy, shape, jnp.float32), much_dy)
    drawn = {"x": x.astype(jnp.bfloat16), "dy": (loud * dy * (SEQUENCES * TOKENS) ** -0.5).astype(jnp.bfloat16)}
    for key, name in zip(kw, NAMES, strict=True):
        w = jax.random.normal(key, SHAPES[name], jnp.float32) * SHAPES[name][1] ** -0.5
        drawn[name] = (w * {"w_gate": 1.0, "w_up": bump(kh, FF, 4.0), "w_down": layers}[name]).astype(jnp.bfloat16)
    for key, name in zip(km, NAMES, strict=True):
        drawn[f"m_{name}"] = 0.1 * jax.random.normal(key, SHAPES[name], jnp.float32)
    for key, name in zip(kv, NAMES, strict=True):
        drawn[f"v_{name}"] = jax.random.uniform(key, SHAPES[name], jnp.float32, 0.005, 0.015)
    return drawn


def matmul(a, w):
    return jnp.dot(a, w, preferred_element_type=jnp.float32).astype(jnp.bfloat16)


def normed(h):
    wide = h.astype(jnp.float32)
    scale = lax.rsqrt(jnp.mean(wide**2, -1, keepdims=True) + 1e-6)
    return (wide * scale).astype(jnp.bfloat16)


def layer(h, w):
    a = normed(h)
    gate = jnp.dot(a, w["w_gate"], preferred_element_type=jnp.float32)
    up = jnp.dot(a, w["w_up"], preferred_element_type=jnp.float32)
    return h + matmul((jax.nn.silu(gate) * up).astype(jnp.bfloat16), w["w_down"])


def adamw(w, m, v, g):
    m = 0.9 * m + 0.1 * g
    v = 0.95 * v + 0.05 * g * g
    step = m * lax.rsqrt(v + 1e-8) + 0.1 * w
    return (w - 0.02 * step).astype(jnp.bfloat16), m, v


def stack(weights, h):
    return lax.scan(lambda h, w: (layer(h, w), None), h, weights)[0]


def reference(x, dy, w_gate, w_up, w_down, m_w_gate, m_w_up, m_w_down, v_w_gate, v_w_up, v_w_down):
    weights = dict(zip(NAMES, (w_gate, w_up, w_down), strict=True))

    def take(so_far, sequence):
        h, by_y = sequence
        _, back = jax.vjp(lambda w: stack(w, h), weights)
        return jax.tree.map(lambda total, term: total + term.astype(jnp.float32), so_far, back(by_y)[0]), None

    none_yet = {name: jnp.zeros(w.shape, jnp.float32) for name, w in weights.items()}
    by_weights, _ = lax.scan(take, none_yet, (x, dy))
    gradients = [by_weights[name].astype(jnp.bfloat16).astype(jnp.float32) for name in NAMES]
    new = [
        adamw(w.astype(jnp.float32), m, v, g)
        for w, m, v, g in zip((w_gate, w_up, w_down), (m_w_gate, m_w_up, m_w_down), (v_w_gate, v_w_up, v_w_down), gradients, strict=True)
    ]
    return tuple(one[which] for which in range(3) for one in new)
```

```python
import functools

import jax
import jax.numpy as jnp
from jax import lax
from jax.experimental import pallas as pl
from jax.experimental.pallas import tpu as pltpu
from jax.sharding import PartitionSpec as P

BF, F32 = jnp.bfloat16, jnp.float32
T, D, FF = 2048, 768, 6144
BN = 512
VMEM_LIMIT = 60 * 1024 * 1024


def normed(h):
    wide = h.astype(F32)
    scale = lax.rsqrt(jnp.mean(wide**2, -1, keepdims=True) + 1e-6)
    return (wide * scale).astype(BF)


def sds(shape, dtype):
    return jax.ShapeDtypeStruct(shape, dtype)


def params(n=1):
    return pltpu.CompilerParams(dimension_semantics=("arbitrary",) * n, vmem_limit_bytes=VMEM_LIMIT)


def cost(matmuls, bytes_):
    return pl.CostEstimate(flops=int(2 * matmuls * T * D * FF), bytes_accessed=int(bytes_), transcendentals=0)


def mm(a, b, ca, cb):
    return lax.dot_general(a, b, (((ca,), (cb,)), ((), ())), preferred_element_type=F32)


def forward_kernel(rows, a_ref, g_ref, u_ref, act_ref):
    for r in range(0, T, rows):
        a = a_ref[r : r + rows, :]
        gate = mm(a, g_ref[0], 1, 0)
        up = mm(a, u_ref[0], 1, 0)
        act_ref[r : r + rows, :] = (gate * jax.nn.sigmoid(gate) * up).astype(BF)


def forward(a, w_gate, w_up, number):
    tile = lambda i: (number, 0, i)
    return pl.pallas_call(
        functools.partial(forward_kernel, 512),
        grid=(FF // BN,),
        in_specs=[
            pl.BlockSpec((T, D), lambda i: (0, 0)),
            pl.BlockSpec((1, D, BN), tile),
            pl.BlockSpec((1, D, BN), tile),
        ],
        out_specs=pl.BlockSpec((T, BN), lambda i: (0, i)),
        out_shape=sds((T, FF), BF),
        compiler_params=params(),
        cost_estimate=cost(2, 50e6),
        name="forward",
    )(a, w_gate, w_up)


def down_kernel(act_ref, w_ref, h_ref, out_ref, a_ref):
    h = h_ref[...] + mm(act_ref[...], w_ref[0], 1, 0).astype(BF)
    out_ref[...] = h
    a_ref[...] = normed(h)


def down(act, w_down, h, number, rows=256):
    return pl.pallas_call(
        down_kernel,
        grid=(T // rows,),
        in_specs=[
            pl.BlockSpec((rows, FF), lambda i: (i, 0)),
            pl.BlockSpec((1, FF, D), lambda i: (number, 0, 0)),
            pl.BlockSpec((rows, D), lambda i: (i, 0)),
        ],
        out_specs=[pl.BlockSpec((rows, D), lambda i: (i, 0))] * 2,
        out_shape=[sds((T, D), BF)] * 2,
        compiler_params=params(),
        cost_estimate=cost(1, 45e6),
        name="down",
    )(act, w_down, h)


def backward_kernel(rows, a_ref, dy_ref, g_ref, u_ref, d_ref, act_ref, dgate_ref, dup_ref):
    for r in range(0, T, rows):
        at = slice(r, r + rows)
        a = a_ref[at, :]
        gate = mm(a, g_ref[0], 1, 0)
        up = mm(a, u_ref[0], 1, 0)
        dact = mm(dy_ref[at, :], d_ref[0], 1, 1).astype(BF).astype(F32)
        sig = jax.nn.sigmoid(gate)
        silu = gate * sig
        act_ref[at, :] = (silu * up).astype(BF)
        dup_ref[at, :] = (dact * silu).astype(BF)
        dgate_ref[at, :] = (dact * up * (sig + silu * (1.0 - sig))).astype(BF)


def backward(a, dy, w_gate, w_up, w_down, number, wide=256):
    tile = lambda i: (number, 0, i)
    whole = pl.BlockSpec((T, D), lambda i: (0, 0))
    out = pl.BlockSpec((T, wide), lambda i: (0, i))
    return pl.pallas_call(
        functools.partial(backward_kernel, 512),
        grid=(FF // wide,),
        in_specs=[
            whole,
            whole,
            pl.BlockSpec((1, D, wide), tile),
            pl.BlockSpec((1, D, wide), tile),
            pl.BlockSpec((1, wide, D), lambda i: (number, i, 0)),
        ],
        out_specs=[out] * 3,
        out_shape=[sds((T, FF), BF)] * 3,
        compiler_params=params(),
        cost_estimate=cost(3, 110e6),
        name="backward",
    )(a, dy, w_gate, w_up, w_down)


def into_kernel(dg_ref, du_ref, g_ref, u_ref, h_ref, dy_ref, out_ref):
    da = mm(dg_ref[...], g_ref[0], 1, 1).astype(BF) + mm(du_ref[...], u_ref[0], 1, 1).astype(BF)
    da, h = da.astype(F32), h_ref[...].astype(F32)
    scale = lax.rsqrt(jnp.mean(h * h, -1, keepdims=True) + 1e-6)
    dh = scale * da - h * (scale * scale * scale) * jnp.mean(da * h, -1, keepdims=True)
    out_ref[...] = dy_ref[...] + dh.astype(BF)


def into(dgate, dup, w_gate, w_up, h, dy, number, rows=256):
    row = pl.BlockSpec((rows, D), lambda i: (i, 0))
    wide = pl.BlockSpec((rows, FF), lambda i: (i, 0))
    w = pl.BlockSpec((1, D, FF), lambda i: (number, 0, 0), pipeline_mode=pl.Buffered(1))
    return pl.pallas_call(
        into_kernel,
        grid=(T // rows,),
        in_specs=[wide, wide, w, w, row, row],
        out_specs=row,
        out_shape=sds((T, D), BF),
        compiler_params=params(),
        cost_estimate=cost(2, 80e6),
        name="into",
    )(dgate, dup, w_gate, w_up, h, dy)


ORDERS = ((4, 2, 1), (2, 1, 4), (1, 4, 2))


def place(j, order):
    first, second, third = order
    bit = lambda b: (j // b) % 2
    return bit(first), 2 * bit(second) + bit(third)


def wide_kernel(where_ref, a_ref, rhs_ref, own_ref, other_ref, flat, lhs):
    @pl.when(pl.program_id(0) == 0)
    def _():
        flat[...] = a_ref[...].T
        core = where_ref[8]
        for q in range(8):
            for side in range(2):
                block = 2 * where_ref[q] + (core if side == 0 else 1 - core)
                lhs[pl.ds(384 * side + 48 * q, 48), :] = flat[pl.ds(pl.multiple_of(block * 48, 16), 48), :]

    whole = mm(lhs[...], rhs_ref[...], 1, 0).astype(BF)
    own_ref[...] = whole[:384].reshape(8, 48, BN)
    other_ref[...] = whole[384:].reshape(8, 48, BN)


def wide_gradient(where, a, rhs):
    part = pl.BlockSpec((8, 48, BN), lambda i, w: (0, 0, i))
    return pl.pallas_call(
        wide_kernel,
        grid_spec=pltpu.PrefetchScalarGridSpec(
            num_scalar_prefetch=1,
            grid=(FF // BN,),
            in_specs=[pl.BlockSpec((T, D), lambda i, w: (0, 0)), pl.BlockSpec((T, BN), lambda i, w: (0, i))],
            out_specs=[part, part],
            scratch_shapes=[pltpu.VMEM((D, T), BF), pltpu.VMEM((D, T), BF)],
        ),
        out_shape=[sds((8, 48, FF), BF)] * 2,
        compiler_params=params(),
        cost_estimate=cost(1, 40e6),
        name="wide",
    )(where, a, rhs)


def tall_kernel(where_ref, act_ref, dy_ref, own_ref, other_ref, whole):
    core = where_ref[8]
    whole[...] = mm(act_ref[...], dy_ref[...], 0, 0).reshape(2, 384, D)
    own_ref[0] = whole[core].astype(BF)
    other_ref[0] = whole[1 - core].astype(BF)


def tall_gradient(where, act, dy):
    part = pl.BlockSpec((1, 384, D), lambda q, w: (q, 0, 0))
    return pl.pallas_call(
        tall_kernel,
        grid_spec=pltpu.PrefetchScalarGridSpec(
            num_scalar_prefetch=1,
            grid=(8,),
            in_specs=[pl.BlockSpec((T, 768), lambda q, w: (0, w[q])), pl.BlockSpec((T, D), lambda q, w: (0, 0))],
            out_specs=[part, part],
            scratch_shapes=[pltpu.VMEM((2, 384, D), F32)],
        ),
        out_shape=[sds((8, 384, D), BF)] * 2,
        compiler_params=params(),
        cost_estimate=cost(1, 40e6),
        name="tall",
    )(where, act, dy)


def pair_kernel(own_ref, got_ref, *refs):
    whole = (own_ref[0].astype(F32) + got_ref[0].astype(F32)).astype(BF)
    rows, columns = whole.shape
    for s in range(rows // 48):
        refs[-1][0, :, s * columns : (s + 1) * columns] = whole[s * 48 : (s + 1) * 48]


def pair_sum(own, got, side, old=None):
    n, r, c = own.shape
    block = pl.BlockSpec((1, r, c), lambda i: (i, 0, 0))
    return pl.pallas_call(
        pair_kernel,
        grid=(n,),
        in_specs=[block, block] + [pl.BlockSpec(memory_space=pl.ANY)] * (old is not None),
        out_specs=pl.BlockSpec((1, 48, FF), lambda i: (i, 0, side)),
        out_shape=sds((n, 48, 3 * FF), BF),
        input_output_aliases={2: 0} if old is not None else {},
        compiler_params=params(),
        cost_estimate=pl.CostEstimate(flops=int(4e8), bytes_accessed=6 * n * r * c, transcendentals=0),
        name="pair_sum",
    )(own, got, *((old,) if old is not None else ()))


def split_kernel(own_ref, got_ref, *refs):
    keeps, sends = refs[:3], refs[3:]
    whole = own_ref[...].astype(F32) + got_ref[...].astype(F32)

    def put(third, piece):
        for j in range(8):
            leaves, at = place(j, ORDERS[third])
            if leaves:
                sends[third][at] = piece[j].astype(BF)
            else:
                keeps[third][at] = piece[j]

    if whole.shape[1] == 48:
        for third in range(3):
            pl.when(pl.program_id(0) // 4 == third)(functools.partial(put, third, whole))
    else:
        for third in range(3):
            put(third, whole[:, :, third * 256 : third * 256 + 256])


def pair_split(own, got):
    _, r, c = own.shape
    if r == 48:
        grid, part = (12,), pl.BlockSpec((8, 48, BN), lambda i: (0, 0, i))
        out = [pl.BlockSpec((4, 48, BN), lambda i, k=k: (0, 0, jnp.clip(i - 4 * k, 0, 3))) for k in range(3)]
    else:
        grid, part = (8,), pl.BlockSpec((8, 48, c), lambda i: (0, i, 0))
        out = [pl.BlockSpec((4, 48, c // 3), lambda i: (0, i, 0))] * 3
        grid, part = (4,), pl.BlockSpec((8, 96, c), lambda i: (0, i, 0))
        out = [pl.BlockSpec((4, 96, c // 3), lambda i: (0, i, 0))] * 3
    return pl.pallas_call(
        split_kernel,
        grid=grid,
        in_specs=[part, part],
        out_specs=out * 2,
        out_shape=[sds((4, r, c // 3), F32)] * 3 + [sds((4, r, c // 3), BF)] * 3,
        compiler_params=params(),
        cost_estimate=pl.CostEstimate(flops=int(4e8), bytes_accessed=7 * 8 * r * c, transcendentals=0),
        name="pair_split",
    )(own, got)


def sum_kernel(n, *refs):
    keeps, gots, outs = refs[:3], refs[3:6], refs[6:]
    half = n // 2
    for k in range(3):
        if n == 1:
            c = keeps[k].shape[-1]
            outs[0][:, k * c : (k + 1) * c] = (keeps[k][0] + gots[k][0].astype(F32)).astype(BF)
        else:
            outs[k][...] = keeps[k][:half] + gots[k][:half].astype(F32)
            outs[3 + k][...] = (keeps[k][half:] + gots[k][half:].astype(F32)).astype(BF)


def add_step(keeps, gots):
    n, r, c = keeps[0].shape
    half = n // 2
    if n == 1:
        steps, rows = 1, r
        shapes = sds((r, 3 * c), BF)
        out_specs = pl.BlockSpec((r, 3 * c), lambda i: (0, 0))
    else:
        steps = 3
        rows = r // steps
        shapes = [sds((half, r, c), F32)] * 3 + [sds((half, r, c), BF)] * 3
        out_specs = [pl.BlockSpec((half, rows, c), lambda i: (0, i, 0))] * 6
    block = pl.BlockSpec((n, rows, c), lambda i: (0, i, 0))
    return pl.pallas_call(
        functools.partial(sum_kernel, n),
        grid=(steps,),
        in_specs=[block] * 6,
        out_specs=out_specs,
        out_shape=shapes,
        compiler_params=params(),
        cost_estimate=pl.CostEstimate(flops=int(4e7 * n), bytes_accessed=n * r * c * 30, transcendentals=0),
        name="add_step",
    )(*keeps, *gots)


def adamw_kernel(folded, w_ref, m_ref, v_ref, g_ref, *refs):
    nw, nm, nv = refs[-3:]

    def put(at, g):
        g = g.astype(F32)
        w = w_ref[0, at].astype(F32)
        m = 0.9 * m_ref[0, at] + 0.1 * g
        v = 0.95 * v_ref[0, at] + 0.05 * g * g
        step = m * lax.rsqrt(v + 1e-8) + 0.1 * w
        nw[0, at] = (w - 0.02 * step).astype(BF)
        nm[0, at] = m
        nv[0, at] = v

    if folded:
        for b in range(g_ref.shape[0] // 48):
            for s in range(8):
                put(pl.ds(b * 384 + s * 48, 48), g_ref[b * 48 : b * 48 + 48, s * D : s * D + D])
    else:
        put(slice(None), g_ref[...])


def adamw(w, m, v, g, number, old=None, side=0):
    _, r, c = w.shape
    folded = c != FF and g.shape[1] == 3 * FF
    steps = 8 if folded else 6
    block = pl.BlockSpec((1, r // steps, c), lambda i: (number, i, 0))
    g_block = (D // steps, FF) if folded else (r // steps, c)
    extra = tuple(old) if old is not None else ()
    return pl.pallas_call(
        functools.partial(adamw_kernel, folded),
        grid=(steps,),
        in_specs=[block] * 3 + [pl.BlockSpec(g_block, lambda i: (i, side))] + [pl.BlockSpec(memory_space=pl.ANY)] * len(extra),
        out_specs=[block] * 3,
        out_shape=[sds(w.shape, BF), sds(w.shape, F32), sds(w.shape, F32)],
        input_output_aliases={4 + i: i for i in range(len(extra))},
        compiler_params=params(),
        cost_estimate=pl.CostEstimate(flops=int(19e9), bytes_accessed=22 * r * c, transcendentals=r * c),
        name="adamw",
    )(w, m, v, g, *extra)


CHIPS, ALL = ("x", "y", "z"), ("x", "y", "z", "core")
NAME = {4: "x", 2: "y", 1: "z"}


def swap(x, axis):
    return lax.ppermute(x, axis, [(0, 1), (1, 0)])


def swap_step(sends, step):
    return [swap(s, NAME[order[step]]) for s, order in zip(sends, ORDERS)]


def gather(g):
    return lax.all_gather(g, ALL, axis=0, tiled=True)


def scatter(g):
    return lax.psum_scatter(g, CHIPS, scatter_dimension=0, tiled=True)[0]


def tie(x, after):
    return lax.optimization_barrier((x, after))[0]


class Line:
    def __init__(self):
        self.last = None

    def __call__(self, f, first, *rest, **kw):
        if self.last is not None:
            if isinstance(first, (list, tuple)):
                first = [tie(first[0], self.last), *first[1:]]
            else:
                first = tie(first, self.last)
        out = f(first, *rest, **kw)
        self.last = out[0] if isinstance(out, (list, tuple)) else out
        return out


def solution(mesh):
    split = jax.sharding.Mesh(mesh.devices.reshape(1, 2, 2, 2, 2), ("rep", *ALL))

    def step(x, dy, w_gate, w_up, w_down, m_gate, m_up, m_down, v_gate, v_up, v_down):
        x, dy = x[0], dy[0]
        chip = 4 * lax.axis_index("x") + 2 * lax.axis_index("y") + lax.axis_index("z")
        core = lax.axis_index("core")
        count = jnp.arange(8, dtype=jnp.int32)
        plain = jnp.concatenate([count, core[None].astype(jnp.int32)])
        nearest = jnp.concatenate([count ^ chip, core[None].astype(jnp.int32)])
        run = Line()
        wide = lambda rhs, a, where: wide_gradient(where, a, rhs)
        tall = lambda act, dy, where: tall_gradient(where, act, dy)

        a0 = normed(x)
        act0 = run(forward, a0, w_gate, w_up, 0)
        h1, a1 = run(down, act0, w_down, x, 0)
        act1, dgate1, dup1 = run(backward, a1, dy, w_gate, w_up, w_down, 1)

        d1, d1_other = run(tall, act1, dy, plain)
        d1_got = swap(d1_other, "core")
        g1, g1_other = run(wide, dgate1, a1, plain)
        g1_got = swap(g1_other, "core")
        u1, u1_other = run(wide, dup1, a1, plain)
        u1_got = swap(u1_other, "core")
        first = run(pair_sum, d1, d1_got, 2)
        first = run(pair_sum, g1, g1_got, 0, first)
        first = scatter(run(pair_sum, u1, u1_got, 1, first))
        by_h = run(into, dgate1, dup1, w_gate, w_up, h1, dy, 1)
        act0, dgate0, dup0 = run(backward, a0, by_h, w_gate, w_up, w_down, 0)
        first = gather(tie(first, act0))

        d0, d0_other = run(tall, act0, by_h, nearest)
        d0_got = swap(d0_other, "core")
        g0, g0_other = run(wide, dgate0, a0, nearest)
        g0_got = swap(g0_other, "core")
        d0 = run(pair_split, d0, d0_got)
        d0_in = swap_step(d0[3:], 0)
        u0, u0_other = run(wide, dup0, a0, nearest)
        u0_got = swap(u0_other, "core")
        g0 = run(pair_split, g0, g0_got)
        g0_in = swap_step(g0[3:], 0)
        u0 = run(pair_split, u0, u0_got)
        u0_in = swap_step(u0[3:], 0)
        d0 = run(add_step, d0[:3], d0_in)
        d0_in = swap_step(d0[3:], 1)
        new_d = run(adamw, w_down, m_down, v_down, first, 1, None, 2)
        d0 = run(add_step, d0[:3], d0_in)
        d0_in = swap_step(d0[3:], 2)
        g0 = run(add_step, g0[:3], g0_in)
        g0_in = swap_step(g0[3:], 1)
        u0 = run(add_step, u0[:3], u0_in)
        u0_in = swap_step(u0[3:], 1)
        d0 = gather(run(add_step, d0[:3], d0_in))
        new_g = run(adamw, w_gate, m_gate, v_gate, first, 1)
        g0 = run(add_step, g0[:3], g0_in)
        g0_in = swap_step(g0[3:], 2)
        u0 = run(add_step, u0[:3], u0_in)
        u0_in = swap_step(u0[3:], 2)
        g0 = gather(run(add_step, g0[:3], g0_in))
        new_u = run(adamw, w_up, m_up, v_up, first, 1, None, 1)
        u0 = gather(run(add_step, u0[:3], u0_in))
        new_d = run(adamw, w_down, m_down, v_down, d0, 0, new_d)
        new_g = run(adamw, w_gate, m_gate, v_gate, g0, 0, new_g)
        new_u = run(adamw, w_up, m_up, v_up, u0, 0, new_u)
        return tuple(one[which] for which in range(3) for one in (new_g, new_u, new_d))

    return jax.shard_map(
        step,
        mesh=split,
        in_specs=(P(("rep", *ALL), None, None),) * 2 + (P(None, None, None),) * 9,
        out_specs=(P("rep", None, None),) * 9,
        check_vma=False,
    )
```

```python
import functools

import jax
import jax.numpy as jnp
from jax import lax
from jax.experimental import pallas as pl
from jax.experimental.pallas import tpu as pltpu
from jax.sharding import PartitionSpec as P

BF, F32 = jnp.bfloat16, jnp.float32
T, D, FF = 2048, 768, 6144
BN = 512
VMEM_LIMIT = 60 * 1024 * 1024


def normed(h):
    wide = h.astype(F32)
    scale = lax.rsqrt(jnp.mean(wide**2, -1, keepdims=True) + 1e-6)
    return (wide * scale).astype(BF)


def sds(shape, dtype):
    return jax.ShapeDtypeStruct(shape, dtype)


def params(n=1):
    return pltpu.CompilerParams(dimension_semantics=("arbitrary",) * n, vmem_limit_bytes=VMEM_LIMIT)


def cost(matmuls, bytes_):
    return pl.CostEstimate(flops=int(2 * matmuls * T * D * FF), bytes_accessed=int(bytes_), transcendentals=0)


def mm(a, b, ca, cb):
    return lax.dot_general(a, b, (((ca,), (cb,)), ((), ())), preferred_element_type=F32)


def forward_kernel(rows, a_ref, g_ref, u_ref, act_ref, gate_ref):
    for r in range(0, T, rows):
        a = a_ref[r : r + rows, :]
        gate = mm(a, g_ref[0], 1, 0)
        up = mm(a, u_ref[0], 1, 0)
        act_ref[r : r + rows, :] = (gate * jax.nn.sigmoid(gate) * up).astype(BF)
        gate_ref[r : r + rows, :] = gate


def forward(a, w_gate, w_up, number):
    tile = lambda i: (number, 0, i)
    return pl.pallas_call(
        functools.partial(forward_kernel, 512),
        grid=(FF // BN,),
        in_specs=[
            pl.BlockSpec((T, D), lambda i: (0, 0)),
            pl.BlockSpec((1, D, BN), tile),
            pl.BlockSpec((1, D, BN), tile),
        ],
        out_specs=[pl.BlockSpec((T, BN), lambda i: (0, i))] * 2,
        out_shape=[sds((T, FF), BF), sds((T, FF), F32)],
        compiler_params=params(),
        cost_estimate=cost(2, 100e6),
        name="forward",
    )(a, w_gate, w_up)


def down_kernel(act_ref, w_ref, h_ref, out_ref, a_ref):
    h = h_ref[...] + mm(act_ref[...], w_ref[0], 1, 0).astype(BF)
    out_ref[...] = h
    a_ref[...] = normed(h)


def down(act, w_down, h, number, rows=256):
    return pl.pallas_call(
        down_kernel,
        grid=(T // rows,),
        in_specs=[
            pl.BlockSpec((rows, FF), lambda i: (i, 0)),
            pl.BlockSpec((1, FF, D), lambda i: (number, 0, 0)),
            pl.BlockSpec((rows, D), lambda i: (i, 0)),
        ],
        out_specs=[pl.BlockSpec((rows, D), lambda i: (i, 0))] * 2,
        out_shape=[sds((T, D), BF)] * 2,
        compiler_params=params(),
        cost_estimate=cost(1, 45e6),
        name="down",
    )(act, w_down, h)


def backward_kernel(rows, a_ref, dy_ref, g_ref, u_ref, d_ref, act_ref, dgate_ref, dup_ref):
    for r in range(0, T, rows):
        at = slice(r, r + rows)
        a = a_ref[at, :]
        gate = mm(a, g_ref[0], 1, 0)
        up = mm(a, u_ref[0], 1, 0)
        dact = mm(dy_ref[at, :], d_ref[0], 1, 1).astype(BF).astype(F32)
        sig = jax.nn.sigmoid(gate)
        silu = gate * sig
        act_ref[at, :] = (silu * up).astype(BF)
        dup_ref[at, :] = (dact * silu).astype(BF)
        dgate_ref[at, :] = (dact * up * (sig + silu * (1.0 - sig))).astype(BF)


def backward(a, dy, w_gate, w_up, w_down, number, wide=256):
    tile = lambda i: (number, 0, i)
    whole = pl.BlockSpec((T, D), lambda i: (0, 0))
    out = pl.BlockSpec((T, wide), lambda i: (0, i))
    return pl.pallas_call(
        functools.partial(backward_kernel, 512),
        grid=(FF // wide,),
        in_specs=[
            whole,
            whole,
            pl.BlockSpec((1, D, wide), tile),
            pl.BlockSpec((1, D, wide), tile),
            pl.BlockSpec((1, wide, D), lambda i: (number, i, 0)),
        ],
        out_specs=[out] * 3,
        out_shape=[sds((T, FF), BF)] * 3,
        compiler_params=params(),
        cost_estimate=cost(3, 110e6),
        name="backward",
    )(a, dy, w_gate, w_up, w_down)


def kept_kernel(rows, a_ref, dy_ref, gate_ref, u_ref, d_ref, dgate_ref, dup_ref):
    for r in range(0, T, rows):
        at = slice(r, r + rows)
        gate = gate_ref[at, :]
        up = mm(a_ref[at, :], u_ref[0], 1, 0)
        dact = mm(dy_ref[at, :], d_ref[0], 1, 1).astype(BF).astype(F32)
        sig = jax.nn.sigmoid(gate)
        silu = gate * sig
        dup_ref[at, :] = (dact * silu).astype(BF)
        dgate_ref[at, :] = (dact * up * (sig + silu * (1.0 - sig))).astype(BF)


def backward_kept(a, dy, gate, w_up, w_down, number, wide=256):
    whole = pl.BlockSpec((T, D), lambda i: (0, 0))
    out = pl.BlockSpec((T, wide), lambda i: (0, i))
    return pl.pallas_call(
        functools.partial(kept_kernel, 512),
        grid=(FF // wide,),
        in_specs=[
            whole,
            whole,
            out,
            pl.BlockSpec((1, D, wide), lambda i: (number, 0, i)),
            pl.BlockSpec((1, wide, D), lambda i: (number, i, 0)),
        ],
        out_specs=[out] * 2,
        out_shape=[sds((T, FF), BF)] * 2,
        compiler_params=params(),
        cost_estimate=cost(2, 130e6),
        name="backward_kept",
    )(a, dy, gate, w_up, w_down)


def into_kernel(dg_ref, du_ref, g_ref, u_ref, h_ref, dy_ref, out_ref):
    da = mm(dg_ref[...], g_ref[0], 1, 1).astype(BF) + mm(du_ref[...], u_ref[0], 1, 1).astype(BF)
    da, h = da.astype(F32), h_ref[...].astype(F32)
    scale = lax.rsqrt(jnp.mean(h * h, -1, keepdims=True) + 1e-6)
    dh = scale * da - h * (scale * scale * scale) * jnp.mean(da * h, -1, keepdims=True)
    out_ref[...] = dy_ref[...] + dh.astype(BF)


def into(dgate, dup, w_gate, w_up, h, dy, number, rows=256):
    row = pl.BlockSpec((rows, D), lambda i: (i, 0))
    wide = pl.BlockSpec((rows, FF), lambda i: (i, 0))
    w = pl.BlockSpec((1, D, FF), lambda i: (number, 0, 0), pipeline_mode=pl.Buffered(1))
    return pl.pallas_call(
        into_kernel,
        grid=(T // rows,),
        in_specs=[wide, wide, w, w, row, row],
        out_specs=row,
        out_shape=sds((T, D), BF),
        compiler_params=params(),
        cost_estimate=cost(2, 80e6),
        name="into",
    )(dgate, dup, w_gate, w_up, h, dy)


ORDERS = ((4, 2, 1), (2, 1, 4), (1, 4, 2))


def place(j, order):
    first, second, third = order
    bit = lambda b: (j // b) % 2
    return bit(first), 2 * bit(second) + bit(third)


def wide_kernel(where_ref, a_ref, rhs_ref, own_ref, other_ref, flat, lhs):
    @pl.when(pl.program_id(0) == 0)
    def _():
        flat[...] = a_ref[...].T
        core = where_ref[8]
        for q in range(8):
            for side in range(2):
                block = 2 * where_ref[q] + (core if side == 0 else 1 - core)
                lhs[pl.ds(384 * side + 48 * q, 48), :] = flat[pl.ds(pl.multiple_of(block * 48, 16), 48), :]

    whole = mm(lhs[...], rhs_ref[...], 1, 0).astype(BF)
    own_ref[...] = whole[:384].reshape(8, 48, BN)
    other_ref[...] = whole[384:].reshape(8, 48, BN)


def wide_gradient(where, a, rhs):
    part = pl.BlockSpec((8, 48, BN), lambda i, w: (0, 0, i))
    return pl.pallas_call(
        wide_kernel,
        grid_spec=pltpu.PrefetchScalarGridSpec(
            num_scalar_prefetch=1,
            grid=(FF // BN,),
            in_specs=[pl.BlockSpec((T, D), lambda i, w: (0, 0)), pl.BlockSpec((T, BN), lambda i, w: (0, i))],
            out_specs=[part, part],
            scratch_shapes=[pltpu.VMEM((D, T), BF), pltpu.VMEM((D, T), BF)],
        ),
        out_shape=[sds((8, 48, FF), BF)] * 2,
        compiler_params=params(),
        cost_estimate=cost(1, 40e6),
        name="wide",
    )(where, a, rhs)


def tall_kernel(where_ref, act_ref, dy_ref, own_ref, other_ref, whole):
    core = where_ref[8]
    whole[...] = mm(act_ref[...], dy_ref[...], 0, 0).reshape(2, 384, D)
    own_ref[0] = whole[core].astype(BF)
    other_ref[0] = whole[1 - core].astype(BF)


def tall_gradient(where, act, dy):
    part = pl.BlockSpec((1, 384, D), lambda q, w: (q, 0, 0))
    return pl.pallas_call(
        tall_kernel,
        grid_spec=pltpu.PrefetchScalarGridSpec(
            num_scalar_prefetch=1,
            grid=(8,),
            in_specs=[pl.BlockSpec((T, 768), lambda q, w: (0, w[q])), pl.BlockSpec((T, D), lambda q, w: (0, 0))],
            out_specs=[part, part],
            scratch_shapes=[pltpu.VMEM((2, 384, D), F32)],
        ),
        out_shape=[sds((8, 384, D), BF)] * 2,
        compiler_params=params(),
        cost_estimate=cost(1, 40e6),
        name="tall",
    )(where, act, dy)


def pair_kernel(own_ref, got_ref, *refs):
    whole = (own_ref[0].astype(F32) + got_ref[0].astype(F32)).astype(BF)
    rows, columns = whole.shape
    for s in range(rows // 48):
        refs[-1][0, :, s * columns : (s + 1) * columns] = whole[s * 48 : (s + 1) * 48]


def pair_sum(own, got, side, old=None):
    n, r, c = own.shape
    block = pl.BlockSpec((1, r, c), lambda i: (i, 0, 0))
    return pl.pallas_call(
        pair_kernel,
        grid=(n,),
        in_specs=[block, block] + [pl.BlockSpec(memory_space=pl.ANY)] * (old is not None),
        out_specs=pl.BlockSpec((1, 48, FF), lambda i: (i, 0, side)),
        out_shape=sds((n, 48, 3 * FF), BF),
        input_output_aliases={2: 0} if old is not None else {},
        compiler_params=params(),
        cost_estimate=pl.CostEstimate(flops=int(4e8), bytes_accessed=6 * n * r * c, transcendentals=0),
        name="pair_sum",
    )(own, got, *((old,) if old is not None else ()))


def one_kernel(own_ref, got_ref, out_ref):
    out_ref[...] = (own_ref[...].astype(F32) + got_ref[...].astype(F32)).astype(BF)


def pair_one(own, got):
    n, r, c = own.shape
    block = pl.BlockSpec((2, r, c), lambda i: (i, 0, 0))
    return pl.pallas_call(
        one_kernel,
        grid=(n // 2,),
        in_specs=[block, block],
        out_specs=block,
        out_shape=sds((n, r, c), BF),
        compiler_params=params(),
        cost_estimate=pl.CostEstimate(flops=int(4e8), bytes_accessed=6 * n * r * c, transcendentals=0),
        name="pair_one",
    )(own, got)


def split_kernel(own_ref, got_ref, *refs):
    keeps, sends = refs[:3], refs[3:]
    whole = own_ref[...].astype(F32) + got_ref[...].astype(F32)

    def put(third, piece):
        for j in range(8):
            leaves, at = place(j, ORDERS[third])
            if leaves:
                sends[third][at] = piece[j].astype(BF)
            else:
                keeps[third][at] = piece[j]

    for third in range(3):
        pl.when(pl.program_id(0) // 2 == third)(functools.partial(put, third, whole))


def pair_split(own, got):
    _, r, c = own.shape
    grid, part = (6,), pl.BlockSpec((8, 48, 1024), lambda i: (0, 0, i))
    out = [pl.BlockSpec((4, 48, 1024), lambda i, k=k: (0, 0, jnp.clip(i - 2 * k, 0, 1))) for k in range(3)]
    return pl.pallas_call(
        split_kernel,
        grid=grid,
        in_specs=[part, part],
        out_specs=out * 2,
        out_shape=[sds((4, r, c // 3), F32)] * 3 + [sds((4, r, c // 3), BF)] * 3,
        compiler_params=params(),
        cost_estimate=pl.CostEstimate(flops=int(4e8), bytes_accessed=7 * 8 * r * c, transcendentals=0),
        name="pair_split",
    )(own, got)


def sum_kernel(n, *refs):
    keeps, gots, outs = refs[:3], refs[3:6], refs[6:]
    half = n // 2
    for k in range(3):
        if n == 1:
            c = keeps[k].shape[-1]
            outs[0][:, k * c : (k + 1) * c] = (keeps[k][0] + gots[k][0].astype(F32)).astype(BF)
        else:
            outs[k][...] = keeps[k][:half] + gots[k][:half].astype(F32)
            outs[3 + k][...] = (keeps[k][half:] + gots[k][half:].astype(F32)).astype(BF)


def add_step(keeps, gots):
    n, r, c = keeps[0].shape
    half = n // 2
    if n == 1:
        steps, rows = 1, r
        shapes = sds((r, 3 * c), BF)
        out_specs = pl.BlockSpec((r, 3 * c), lambda i: (0, 0))
    else:
        steps = 3
        rows = r // steps
        shapes = [sds((half, r, c), F32)] * 3 + [sds((half, r, c), BF)] * 3
        out_specs = [pl.BlockSpec((half, rows, c), lambda i: (0, i, 0))] * 6
    block = pl.BlockSpec((n, rows, c), lambda i: (0, i, 0))
    return pl.pallas_call(
        functools.partial(sum_kernel, n),
        grid=(steps,),
        in_specs=[block] * 6,
        out_specs=out_specs,
        out_shape=shapes,
        compiler_params=params(),
        cost_estimate=pl.CostEstimate(flops=int(4e7 * n), bytes_accessed=n * r * c * 30, transcendentals=0),
        name="add_step",
    )(*keeps, *gots)


def adamw_kernel(folded, w_ref, m_ref, v_ref, g_ref, *refs):
    nw, nm, nv = refs[-3:]

    def put(at, g):
        g = g.astype(F32)
        w = w_ref[0, at].astype(F32)
        m = 0.9 * m_ref[0, at] + 0.1 * g
        v = 0.95 * v_ref[0, at] + 0.05 * g * g
        step = m * lax.rsqrt(v + 1e-8) + 0.1 * w
        nw[0, at] = (w - 0.02 * step).astype(BF)
        nm[0, at] = m
        nv[0, at] = v

    if folded:
        for b in range(g_ref.shape[0] // 48):
            for s in range(8):
                put(pl.ds(b * 384 + s * 48, 48), g_ref[b * 48 : b * 48 + 48, s * D : s * D + D])
    else:
        put(slice(None), g_ref[...])


def adamw(w, m, v, g, number, old=None, side=0):
    _, r, c = w.shape
    folded = c != FF and g.shape[1] == 3 * FF
    steps = 8 if folded else 6
    block = pl.BlockSpec((1, r // steps, c), lambda i: (number, i, 0))
    g_block = (D // steps, FF) if folded else (r // steps, c)
    extra = tuple(old) if old is not None else ()
    return pl.pallas_call(
        functools.partial(adamw_kernel, folded),
        grid=(steps,),
        in_specs=[block] * 3 + [pl.BlockSpec(g_block, lambda i: (i, side))] + [pl.BlockSpec(memory_space=pl.ANY)] * len(extra),
        out_specs=[block] * 3,
        out_shape=[sds(w.shape, BF), sds(w.shape, F32), sds(w.shape, F32)],
        input_output_aliases={4 + i: i for i in range(len(extra))},
        compiler_params=params(),
        cost_estimate=pl.CostEstimate(flops=int(19e9), bytes_accessed=22 * r * c, transcendentals=r * c),
        name="adamw",
    )(w, m, v, g, *extra)


CHIPS, ALL = ("x", "y", "z"), ("x", "y", "z", "core")
NAME = {4: "x", 2: "y", 1: "z"}


def swap(x, axis):
    return lax.ppermute(x, axis, [(0, 1), (1, 0)])


def swap_step(sends, step):
    return [swap(s, NAME[order[step]]) for s, order in zip(sends, ORDERS)]


def gather(g):
    return lax.all_gather(g, ALL, axis=0, tiled=True)


def scatter(g):
    return lax.psum_scatter(g, CHIPS, scatter_dimension=0, tiled=True)[0]


def tie(x, after):
    return lax.optimization_barrier((x, after))[0]


class Line:
    def __init__(self):
        self.last = None

    def __call__(self, f, first, *rest, **kw):
        if self.last is not None:
            if isinstance(first, (list, tuple)):
                first = [tie(first[0], self.last), *first[1:]]
            else:
                first = tie(first, self.last)
        out = f(first, *rest, **kw)
        self.last = out[0] if isinstance(out, (list, tuple)) else out
        return out


def solution(mesh):
    split = jax.sharding.Mesh(mesh.devices.reshape(1, 2, 2, 2, 2), ("rep", *ALL))

    def step(x, dy, w_gate, w_up, w_down, m_gate, m_up, m_down, v_gate, v_up, v_down):
        x, dy = x[0], dy[0]
        chip = 4 * lax.axis_index("x") + 2 * lax.axis_index("y") + lax.axis_index("z")
        core = lax.axis_index("core")
        count = jnp.arange(8, dtype=jnp.int32)
        plain = jnp.concatenate([count, core[None].astype(jnp.int32)])
        nearest = jnp.concatenate([count ^ chip, core[None].astype(jnp.int32)])
        run = Line()
        wide = lambda rhs, a, where: wide_gradient(where, a, rhs)
        tall = lambda act, dy, where: tall_gradient(where, act, dy)

        a0 = normed(x)
        act0, gate0 = run(forward, a0, w_gate, w_up, 0)
        h1, a1 = run(down, act0, w_down, x, 0)
        act1, dgate1, dup1 = run(backward, a1, dy, w_gate, w_up, w_down, 1)

        d1, d1_other = run(tall, act1, dy, plain)
        d1_got = swap(d1_other, "core")
        g1, g1_other = run(wide, dgate1, a1, plain)
        g1_got = swap(g1_other, "core")
        u1, u1_other = run(wide, dup1, a1, plain)
        u1_got = swap(u1_other, "core")
        first = run(pair_sum, d1, d1_got, 2)
        first = run(pair_sum, g1, g1_got, 0, first)
        first = scatter(run(pair_sum, u1, u1_got, 1, first))
        by_h = run(into, dgate1, dup1, w_gate, w_up, h1, dy, 1)
        dgate0, dup0 = run(backward_kept, a0, by_h, gate0, w_up, w_down, 0)
        first = gather(tie(first, dgate0))

        d0, d0_other = run(tall, act0, by_h, plain)
        d0_got = swap(d0_other, "core")
        g0, g0_other = run(wide, dgate0, a0, nearest)
        g0_got = swap(g0_other, "core")
        d0 = run(pair_one, d0, d0_got)
        u0, u0_other = run(wide, dup0, a0, nearest)
        u0_got = swap(u0_other, "core")
        g0 = run(pair_split, g0, g0_got)
        g0_in = swap_step(g0[3:], 0)
        u0 = run(pair_split, u0, u0_got)
        u0_in = swap_step(u0[3:], 0)
        g0 = run(add_step, g0[:3], g0_in)
        g0_in = swap_step(g0[3:], 1)
        d0 = scatter(tie(tie(d0, run.last), first))
        new_d = run(adamw, w_down, m_down, v_down, first, 1, None, 2)
        u0 = run(add_step, u0[:3], u0_in)
        u0_in = swap_step(u0[3:], 1)
        g0 = run(add_step, g0[:3], g0_in)
        g0_in = swap_step(g0[3:], 2)
        run.last = d0
        d0 = gather(tie(d0, g0[0]))
        new_g = run(adamw, w_gate, m_gate, v_gate, first, 1)
        g0 = gather(run(add_step, g0[:3], g0_in))
        u0 = run(add_step, u0[:3], u0_in)
        u0_in = swap_step(u0[3:], 2)
        new_u = run(adamw, w_up, m_up, v_up, first, 1, None, 1)
        u0 = gather(run(add_step, u0[:3], u0_in))
        new_d = run(adamw, w_down, m_down, v_down, d0, 0, new_d)
        new_g = run(adamw, w_gate, m_gate, v_gate, g0, 0, new_g)
        new_u = run(adamw, w_up, m_up, v_up, u0, 0, new_u)
        return tuple(one[which] for which in range(3) for one in (new_g, new_u, new_d))

    return jax.shard_map(
        step,
        mesh=split,
        in_specs=(P(("rep", *ALL), None, None),) * 2 + (P(None, None, None),) * 9,
        out_specs=(P("rep", None, None),) * 9,
        check_vma=False,
    )
```
